16 devices in a mesh: data: 16 (over z, y, x, core).
Axes of the slice: x: 2, y: 2, z: 2, core: 2. Of those that a mesh axis runs over, the one named last changes fastest.
Arguments:
- h_a: bfloat16 [16384, 384], P('data')
- h_b: bfloat16 [16384, 384], P('data')
- w_one: bfloat16 [384, 2048], replicated
- w_two: bfloat16 [2048, 2048], replicated
- w_three: bfloat16 [2048, 2048], replicated
- gain_one: float32 [2048], replicated
- bias_one: float32 [2048], replicated
- gain_two: float32 [2048], replicated
- bias_two: float32 [2048], replicated
Outputs:
- output 1: float32 [], replicated
- output 2: float32 [384, 2048], replicated
- output 3: float32 [2048, 2048], replicated
- output 4: float32 [2048, 2048], replicated
- output 5: float32 [2048], replicated
- output 6: float32 [2048], replicated
- output 7: float32 [2048], replicated
- output 8: float32 [2048], replicated
All inputs are finite; a program needn't handle non-finite values.
Results may differ from the reference program's by a relative error of at most 0.001.
Values are sent between devices in bfloat16 or wider.
A program may use at most 1 GiB of HBM per device.

```python
import jax
import jax.numpy as jnp
from jax import lax

GROUP_DEVS = 16
ROWS_DEV = 1024
FEAT_DIM = 384
PROJ_DIM = 2048

ALL_ROWS = GROUP_DEVS * ROWS_DEV
BN_EPS = 1e-5
STD_EPS = 1e-4
INV_WEIGHT = 2.0
VAR_WEIGHT = 1.0
COV_WEIGHT = 2.0


def setup_inputs(seed: int = 0) -> dict:
    key_list = jax.random.split(jax.random.key(seed), 11)
    shard_shape = (GROUP_DEVS, ROWS_DEV, FEAT_DIM)
    stat_shape = (GROUP_DEVS, 1, FEAT_DIM)
    base_a = jax.random.normal(key_list[0], shard_shape, jnp.float32)
    base_b = 0.8 * base_a + 0.6 * jax.random.normal(key_list[1], shard_shape, jnp.float32)
    shard_off = 0.6 * jax.random.normal(key_list[2], stat_shape, jnp.float32)
    shard_scale = jnp.exp(0.3 * jax.random.normal(key_list[3], stat_shape, jnp.float32))
    h_a = ((base_a + shard_off) * shard_scale).reshape(ALL_ROWS, FEAT_DIM).astype(jnp.bfloat16)
    h_b = ((base_b + shard_off) * shard_scale).reshape(ALL_ROWS, FEAT_DIM).astype(jnp.bfloat16)
    w_one = (jax.random.normal(key_list[4], (FEAT_DIM, PROJ_DIM), jnp.float32) * FEAT_DIM ** -0.5).astype(jnp.bfloat16)
    w_two = (jax.random.normal(key_list[5], (PROJ_DIM, PROJ_DIM), jnp.float32) * PROJ_DIM ** -0.5).astype(jnp.bfloat16)
    w_three = (jax.random.normal(key_list[6], (PROJ_DIM, PROJ_DIM), jnp.float32) * (0.7 * PROJ_DIM ** -0.5)).astype(jnp.bfloat16)
    gain_one = 1.0 + 0.3 * jax.random.normal(key_list[7], (PROJ_DIM,), jnp.float32)
    bias_one = 0.3 * jax.random.normal(key_list[8], (PROJ_DIM,), jnp.float32)
    gain_two = 1.0 + 0.3 * jax.random.normal(key_list[9], (PROJ_DIM,), jnp.float32)
    bias_two = 0.3 * jax.random.normal(key_list[10], (PROJ_DIM,), jnp.float32)
    return {'h_a': h_a, 'h_b': h_b, 'w_one': w_one, 'w_two': w_two, 'w_three': w_three,
            'gain_one': gain_one, 'bias_one': bias_one, 'gain_two': gain_two, 'bias_two': bias_two}


def layer_forward(x_in, weight, gain_vec, bias_vec):
    pre_act = jnp.dot(x_in, weight, preferred_element_type=jnp.float32)
    centered = pre_act - jnp.mean(pre_act, axis=0)
    inv_std = lax.rsqrt(jnp.mean(centered * centered, axis=0) + BN_EPS)
    normed = centered * inv_std
    act_val = gain_vec * normed + bias_vec
    return jnp.maximum(act_val, 0.0).astype(jnp.bfloat16), normed, act_val, inv_std


def layer_backward(d_out, normed, act_val, inv_std, gain_vec):
    d_act = jnp.where(act_val > 0.0, d_out, 0.0)
    sum_d = jnp.sum(d_act, axis=0)
    sum_dn = jnp.sum(d_act * normed, axis=0)
    d_pre = inv_std * gain_vec * (d_act - sum_d / ALL_ROWS - normed * (sum_dn / ALL_ROWS))
    return d_pre.astype(jnp.bfloat16), sum_dn, sum_d


def view_forward(view_feats, w_one, w_two, w_three, gain_one, bias_one, gain_two, bias_two):
    hidden_one, normed_one, act_one, inv_one = layer_forward(view_feats, w_one, gain_one, bias_one)
    hidden_two, normed_two, act_two, inv_two = layer_forward(hidden_one, w_two, gain_two, bias_two)
    z_view = jnp.dot(hidden_two, w_three, preferred_element_type=jnp.float32).astype(jnp.bfloat16)
    return z_view, (hidden_one, normed_one, act_one, inv_one, hidden_two, normed_two, act_two, inv_two)


def branch_terms(z_view):
    z_float = z_view.astype(jnp.float32)
    centered = z_float - jnp.mean(z_float, axis=0)
    cov_mat = jnp.dot(centered.T, centered) / (ALL_ROWS - 1)
    diag_var = jnp.diagonal(cov_mat)
    std_vec = jnp.sqrt(diag_var + STD_EPS)
    off_diag = cov_mat - jnp.diag(diag_var)
    hinge_on = (std_vec < 1.0).astype(jnp.float32)
    term_val = VAR_WEIGHT * jnp.sum(jnp.maximum(1.0 - std_vec, 0.0)) + COV_WEIGHT * jnp.sum(off_diag * off_diag)
    grad_cov = 2.0 * COV_WEIGHT * off_diag - jnp.diag(VAR_WEIGHT * hinge_on / (2.0 * std_vec))
    grad_hat = grad_cov.astype(jnp.bfloat16).astype(jnp.float32)
    grad_z = (2.0 / (ALL_ROWS - 1)) * jnp.dot(centered, grad_hat)
    return term_val, grad_z


def view_backward(view_feats, d_z, saved, w_two, w_three, gain_one, gain_two):
    hidden_one, normed_one, act_one, inv_one, hidden_two, normed_two, act_two, inv_two = saved
    grad_three = jnp.dot(hidden_two.T, d_z, preferred_element_type=jnp.float32)
    d_hidden_two = jnp.dot(d_z, w_three.T, preferred_element_type=jnp.float32)
    d_pre_two, gain_grad_two, bias_grad_two = layer_backward(d_hidden_two, normed_two, act_two, inv_two, gain_two)
    grad_two = jnp.dot(hidden_one.T, d_pre_two, preferred_element_type=jnp.float32)
    d_hidden_one = jnp.dot(d_pre_two, w_two.T, preferred_element_type=jnp.float32)
    d_pre_one, gain_grad_one, bias_grad_one = layer_backward(d_hidden_one, normed_one, act_one, inv_one, gain_one)
    grad_one = jnp.dot(view_feats.T, d_pre_one, preferred_element_type=jnp.float32)
    return grad_one, grad_two, grad_three, gain_grad_one, bias_grad_one, gain_grad_two, bias_grad_two


def reference(h_a, h_b, w_one, w_two, w_three, gain_one, bias_one, gain_two, bias_two):
    z_a, saved_a = view_forward(h_a, w_one, w_two, w_three, gain_one, bias_one, gain_two, bias_two)
    z_b, saved_b = view_forward(h_b, w_one, w_two, w_three, gain_one, bias_one, gain_two, bias_two)
    term_a, grad_za = branch_terms(z_a)
    term_b, grad_zb = branch_terms(z_b)
    z_diff = z_a.astype(jnp.float32) - z_b.astype(jnp.float32)
    loss_val = INV_WEIGHT * jnp.sum(z_diff * z_diff) / ALL_ROWS + term_a + term_b
    d_inv = (2.0 * INV_WEIGHT / ALL_ROWS) * z_diff
    d_za = (grad_za + d_inv).astype(jnp.bfloat16)
    d_zb = (grad_zb - d_inv).astype(jnp.bfloat16)
    back_a = view_backward(h_a, d_za, saved_a, w_two, w_three, gain_one, gain_two)
    back_b = view_backward(h_b, d_zb, saved_b, w_two, w_three, gain_one, gain_two)
    summed = [part_a + part_b for part_a, part_b in zip(back_a, back_b)]
    return (loss_val, summed[0], summed[1], summed[2], summed[3], summed[4], summed[5], summed[6])
```

```python
import jax
import jax.numpy as jnp
from jax import lax
from jax.experimental import pallas as pl
from jax.experimental.pallas import tpu as pltpu
from jax.sharding import PartitionSpec as P

BN_EPS = 1e-5
STD_EPS = 1e-4
INV_WEIGHT = 2.0
VAR_WEIGHT = 1.0
COV_WEIGHT = 2.0

N_DEV = 16
ROWS = 1024
DIM = 2048
ALL_ROWS = N_DEV * ROWS
MESH = pl.DeviceIdType.MESH
VMEM_LIMIT = 64 * 1024 * 1024 - 128 * 1024

ORDERS = ((0, 1, 2), (1, 2, 0), (2, 0, 1))
Q_ORDER = (7, 6, 5, 3, 4, 2, 1, 0)


def sent_stage(q, k):
    for s, d in enumerate(ORDERS[k]):
        if (q >> d) & 1:
            return s
    return 3


def last_stage(q, k):
    last = -1
    for s, d in enumerate(ORDERS[k]):
        if (q >> d) & 1:
            last = s
    return last


class Place:
    def __init__(self):
        self.me = lax.axis_index('data')
        self.core = self.me % 2
        self.bits = ((self.me // 2) % 2, (self.me // 4) % 2, self.me // 8)
        self.partner = self.me + 1 - 2 * self.core
        self.near = tuple(self.me + (2 << d) - (4 << d) * self.bits[d] for d in range(3))

    def chip(self, q):
        p = 0
        for d in range(3):
            b = self.bits[d]
            p = p + ((1 - b) if (q >> d) & 1 else b) * (1 << d)
        return p


def entry_barrier(me):
    sem = pltpu.get_barrier_semaphore()
    for k in range(1, N_DEV):
        pl.semaphore_signal(sem, inc=1, device_id=((me + k) % N_DEV,), device_id_type=MESH)
    pl.semaphore_wait(sem, N_DEV - 1)


def rcopy(src, dst, ssem, rsem, dev):
    return pltpu.make_async_remote_copy(src_ref=src, dst_ref=dst, send_sem=ssem, recv_sem=rsem,
                                        device_id=(dev,), device_id_type=MESH)


def lanes(i):
    return pl.ds(pl.multiple_of(i * 128, 128), 128)


class SmallSum:
    def __init__(self, me, x_ref, o_ref, slots, sems):
        self.me, self.x, self.o, self.slots, self.sems = me, x_ref, o_ref, slots, sems

    def out_copy(self, k):
        peer = (self.me + k) % N_DEV
        return rcopy(self.x.at[:, lanes(peer)], self.slots.at[self.me], self.sems.at[0, peer],
                     self.sems.at[1, self.me], peer)

    def in_copy(self, k):
        src = (self.me + k) % N_DEV
        return rcopy(self.x.at[:, lanes(src)], self.slots.at[src], self.sems.at[0, src], self.sems.at[1, src], src)

    def out_bcast(self, k):
        peer = (self.me + k) % N_DEV
        mine = self.o.at[:, lanes(self.me)]
        return rcopy(mine, mine, self.sems.at[2, peer], self.sems.at[3, self.me], peer)

    def in_bcast(self, k):
        src = (self.me + k) % N_DEV
        theirs = self.o.at[:, lanes(src)]
        return rcopy(theirs, theirs, self.sems.at[2, src], self.sems.at[3, src], src)

    def start(self):
        for k in range(1, N_DEV):
            self.out_copy(k).start()
        self.slots[self.me] = self.x[:, lanes(self.me)]

    def middle(self):
        for k in range(1, N_DEV):
            self.in_copy(k).wait_recv()
        total = self.slots[0]
        for s in range(1, N_DEV):
            total = total + self.slots[s]
        self.o[:, lanes(self.me)] = total
        for k in range(1, N_DEV):
            self.out_bcast(k).start()

    def finish(self):
        for k in range(1, N_DEV):
            self.in_bcast(k).wait_recv()
        for k in range(1, N_DEV):
            self.out_copy(k).wait_send()
            self.out_bcast(k).wait_send()


SMALL_SCRATCH = [pltpu.VMEM((N_DEV, 8, 128), jnp.float32), pltpu.SemaphoreType.DMA((4, N_DEV))]


def small_sum_kernel(x_ref, o_ref, slots, sems):
    me = lax.axis_index('data')
    entry_barrier(me)
    s = SmallSum(me, x_ref, o_ref, slots, sems)
    s.start()
    s.middle()
    s.finish()


def small_sum(x, cid):
    vm = pl.BlockSpec(memory_space=pltpu.VMEM)
    return pl.pallas_call(
        small_sum_kernel, out_shape=jax.ShapeDtypeStruct((8, DIM), jnp.float32),
        in_specs=[vm], out_specs=vm, scratch_shapes=SMALL_SCRATCH,
        compiler_params=pltpu.CompilerParams(collective_id=cid, has_side_effects=True),
        cost_estimate=pl.CostEstimate(flops=8_000_000, bytes_accessed=131072, transcendentals=0),
        name='small_sum')(x)


class Reduce:
    def __init__(self, place, own, land, ssem, rsem):
        self.place, self.own, self.land, self.ssem, self.rsem = place, own, land, ssem, rsem

    def copy(self, q, k):
        s = sent_stage(q, k)
        d = ORDERS[k][s]
        dst = q & ~(1 << d)
        return rcopy(self.own(q, k), self.land(s, dst, k), self.ssem.at[k, q], self.rsem.at[k, 8 * s + dst],
                     self.place.near[d])

    def arrive(self, q, k, s):
        self.copy(q | (1 << ORDERS[k][s]), k).wait_recv()
        own = self.own(q, k)
        own[...] = own[...] + self.land(s, q, k)[...]

    def stage(self, stage):
        for q in Q_ORDER:
            for k in range(3):
                if sent_stage(q, k) == stage:
                    for s in range(stage):
                        self.arrive(q, k, s)
                    if stage < 3:
                        self.copy(q, k).start()

    def drain(self):
        for k in range(3):
            for q in range(1, 8):
                self.copy(q, k).wait_send()


class Spread:
    def __init__(self, place, piece, ssem, rsem, csend, crecv, mine=None, lsem=None):
        self.place, self.piece, self.mine, self.lsem = place, piece, mine, lsem
        self.ssem, self.rsem, self.csend, self.crecv = ssem, rsem, csend, crecv

    def source(self, q, k):
        if q == 0 and self.mine is not None:
            return self.mine(k)
        return self.piece(self.place.chip(q), self.place.core, k)

    def copy(self, q, k, u):
        d = ORDERS[k][u]
        ref = self.piece(self.place.chip(q), self.place.core, k)
        return rcopy(self.source(q, k), ref, self.ssem.at[k, 3 * q + u], self.rsem.at[k, q | (1 << d)],
                     self.place.near[d])

    def to_partner(self, q, k):
        ref = self.piece(self.place.chip(q), self.place.core, k)
        return rcopy(self.source(q, k), ref, self.csend.at[k, q], self.crecv.at[k, q], self.place.partner)

    def keep(self, k):
        ref = self.piece(self.place.chip(0), self.place.core, k)
        return pltpu.make_async_copy(self.mine(k), ref, self.lsem.at[k])

    def from_partner(self, q, k):
        ref = self.piece(self.place.chip(q), 1 - self.place.core, k)
        return rcopy(ref, ref, self.csend.at[k, q], self.crecv.at[k, q], self.place.partner)

    def start(self, k):
        for u in range(3):
            self.copy(0, k, u).start()
        self.to_partner(0, k).start()
        if self.mine is not None:
            self.keep(k).start()

    def run(self, stages=(0, 1, 2)):
        for stage in stages:
            for q in range(1, 8):
                for k in range(3):
                    if last_stage(q, k) != stage:
                        continue
                    d = ORDERS[k][stage]
                    ref = self.piece(self.place.chip(q), self.place.core, k)
                    rcopy(ref, ref, self.ssem.at[k, 3 * q], self.rsem.at[k, q], self.place.near[d]).wait_recv()
                    for u in range(stage + 1, 3):
                        self.copy(q, k, u).start()
                    self.to_partner(q, k).start()

    def finish(self):
        for q in range(8):
            for k in range(3):
                self.from_partner(q, k).wait_recv()
        for k in range(3):
            if self.mine is not None:
                self.keep(k).wait()
        for q in range(8):
            for k in range(3):
                for u in range(last_stage(q, k) + 1, 3):
                    self.copy(q, k, u).wait_send()
                self.to_partner(q, k).wait_send()


def land_slot(s, q, k):
    order = [x for x in range(8) if sent_stage(x, k) > s]
    return (0, 4, 6)[s] + order.index(q)


def gram_kernel(z_ref, st_ref, pack_ref, tot_ref, loss_ref, gbuf, cbuf, rbuf, slots, sems, csem, rs_s, rs_r,
                ag_s, ag_r, agc_s, agc_r):
    place = Place()
    me, core = place.me, place.core
    entry_barrier(me)
    small = SmallSum(me, st_ref, tot_ref, slots, sems)
    small.start()

    def to_partner(q):
        return rcopy(gbuf.at[1, q, pl.ds(0, 9)], cbuf.at[q], csem.at[0, q], csem.at[1, q], place.partner)

    red = Reduce(place, lambda q, k: gbuf.at[0, q, pl.ds(3 * k, 3)],
                 lambda s, q, k: rbuf.at[k, land_slot(s, q, k)], rs_s, rs_r)

    def core_sum(q):
        to_partner(q).wait_recv()
        mine = gbuf.at[0, q, pl.ds(0, 9)]
        mine[...] = mine[...] + cbuf[q]
        for k in range(3):
            if sent_stage(q, k) == 0:
                red.copy(q, k).start()

    for i, q in enumerate(Q_ORDER):
        p = place.chip(q)

        @pl.loop(0, 2)
        def _(v):
            left = z_ref[v, :, pl.ds(pl.multiple_of(p * 256, 256), 256)]

            @pl.loop(0, 5)
            def _(b):
                right = z_ref[v, :, pl.ds(pl.multiple_of(((p + b) % 8) * 256, 256), 256)]
                out = lax.dot_general(left, right, (((0,), (0,)), ((), ())), preferred_element_type=jnp.float32)
                gbuf[core, q, 2 * b, v] = out[:128, :128]
                gbuf[core, q, 2 * b + 1, v] = out[:128, 128:]
                gbuf[1 - core, q, (2 * b + 9) % 10, v] = out[128:, :128]
                gbuf[1 - core, q, 2 * b, v] = out[128:, 128:]

        to_partner(q).start()
        if i == 1:
            small.middle()
        if i > 0:
            core_sum(Q_ORDER[i - 1])
    core_sum(0)
    for s in (1, 2, 3):
        red.stage(s)
    small.finish()

    ag = Spread(place, lambda p, c, k: pack_ref.at[2 * p + c, pl.ds(3 * k, 3)], ag_s, ag_r, agc_s, agc_r)
    eye = lax.broadcasted_iota(jnp.int32, (128, 128), 0) == lax.broadcasted_iota(jnp.int32, (128, 128), 1)
    acc = jnp.zeros((128, 128), jnp.float32)
    mu_rows = [jnp.transpose(jnp.broadcast_to(tot_ref[pl.ds(v, 1), lanes(me)] / ALL_ROWS, (128, 128))) for v in range(2)]
    for j in range(9):
        for v in range(2):
            mu_cols = tot_ref[pl.ds(v, 1), lanes((me + j) % N_DEV)] / ALL_ROWS
            cov = (gbuf[0, 0, j, v] - ALL_ROWS * mu_rows[v] * mu_cols) / (ALL_ROWS - 1)
            grad = (2.0 * COV_WEIGHT) * cov
            if j == 0:
                std = jnp.sqrt(jnp.where(eye, cov, 1.0) + STD_EPS)
                hinge = (std < 1.0).astype(jnp.float32)
                acc = acc + jnp.where(eye, VAR_WEIGHT * jnp.maximum(1.0 - std, 0.0), COV_WEIGHT * cov * cov)
                grad = jnp.where(eye, -VAR_WEIGHT * hinge / (2.0 * std), grad)
            else:
                acc = acc + (COV_WEIGHT * (2.0 if j < 8 else 1.0)) * cov * cov
            pack_ref[me, j, v] = grad.astype(jnp.bfloat16)
        if j % 3 == 2:
            ag.start(j // 3)
    part = acc[0:8]
    for r in range(1, 16):
        part = part + acc[8 * r:8 * r + 8]
    loss_ref[...] = part
    ag.run()
    ag.finish()
    for q in range(8):
        to_partner(q).wait_send()
    red.drain()


def gram_loss(z, stats, cid):
    vm = pl.BlockSpec(memory_space=pltpu.VMEM)
    dma = pltpu.SemaphoreType.DMA
    return pl.pallas_call(
        gram_kernel,
        out_shape=(jax.ShapeDtypeStruct((N_DEV, 9, 2, 128, 128), jnp.bfloat16),
                   jax.ShapeDtypeStruct((8, DIM), jnp.float32),
                   jax.ShapeDtypeStruct((8, 128), jnp.float32)),
        in_specs=[vm, vm], out_specs=(vm, vm, vm),
        scratch_shapes=[pltpu.VMEM((2, 8, 10, 2, 128, 128), jnp.float32),
                        pltpu.VMEM((8, 9, 2, 128, 128), jnp.float32),
                        pltpu.VMEM((3, 7, 3, 2, 128, 128), jnp.float32)] + SMALL_SCRATCH
                       + [dma((2, 8)), dma((3, 8)), dma((3, 24)), dma((3, 24)), dma((3, 8)), dma((3, 8)), dma((3, 8))],
        compiler_params=pltpu.CompilerParams(collective_id=cid, has_side_effects=True, vmem_limit_bytes=VMEM_LIMIT),
        cost_estimate=pl.CostEstimate(flops=60_000_000_000, bytes_accessed=20_000_000, transcendentals=0),
        name='gram_loss')(z, stats)


def dz_kernel(z_ref, pack_ref, tot_ref, o_ref, gcol):
    v, t = pl.program_id(0), pl.program_id(1)
    for h in range(2):
        c = 2 * t + h
        col = pl.ds(128 * h, 128)
        for d in range(16):
            r = (c + 16 - d) % 16
            rows = pl.ds(pl.multiple_of(r * 128, 128), 128)
            if d <= 8:
                gcol[rows, col] = pack_ref[r, d, v]
            else:
                gcol[rows, col] = jnp.transpose(pack_ref[c, 16 - d, v])
    mu = jnp.broadcast_to(tot_ref[pl.ds(v, 1), :] / ALL_ROWS, (16, DIM))
    high = mu.astype(jnp.bfloat16).astype(jnp.float32)
    mid = (mu - high).astype(jnp.bfloat16).astype(jnp.float32)
    low = mu - high - mid
    row = lax.broadcasted_iota(jnp.int32, (16, DIM), 0)
    terms = jnp.where(row == 0, high, jnp.where(row == 1, mid, jnp.where(row == 2, low, 0.0))).astype(jnp.bfloat16)
    mean = jnp.sum(jnp.dot(terms, gcol[...], preferred_element_type=jnp.float32), axis=0, keepdims=True)
    sign = (1 - 2 * v).astype(jnp.float32) * (2.0 * INV_WEIGHT / ALL_ROWS)
    cols = pl.ds(pl.multiple_of(t * 256, 256), 256)

    @pl.loop(0, 4)
    def _(m):
        rows = pl.ds(pl.multiple_of(m * 256, 256), 256)
        acc = jnp.dot(z_ref[v, rows, :], gcol[...], preferred_element_type=jnp.float32)
        diff = z_ref[0, rows, cols].astype(jnp.float32) - z_ref[1, rows, cols].astype(jnp.float32)
        o_ref[0, rows, :] = ((2.0 / (ALL_ROWS - 1)) * (acc - mean) + sign * diff).astype(jnp.bfloat16)


def dz_call(z, pack, tot):
    full = lambda shape: pl.BlockSpec(shape, lambda v, t: (0,) * len(shape), pipeline_mode=pl.Buffered(1))
    return pl.pallas_call(
        dz_kernel, grid=(2, 8), out_shape=jax.ShapeDtypeStruct((2, ROWS, DIM), jnp.bfloat16),
        in_specs=[full((2, ROWS, DIM)), full((N_DEV, 9, 2, 128, 128)), full((8, DIM))],
        out_specs=pl.BlockSpec((1, ROWS, 256), lambda v, t: (v, 0, t)),
        scratch_shapes=[pltpu.VMEM((DIM, 256), jnp.bfloat16)],
        compiler_params=pltpu.CompilerParams(vmem_limit_bytes=40 * 1024 * 1024,
                                             dimension_semantics=('arbitrary', 'arbitrary')),
        cost_estimate=pl.CostEstimate(flops=2 * 2 * ROWS * DIM * DIM, bytes_accessed=27_000_000, transcendentals=0),
        name='dz')(z, pack, tot)


COLS = ((0, 640), (640, 640), (1280, 768))


def wgrad_kernel(x_ref, d_ref, w_ref, o_ref, p_ref, xt, part, cbuf, rbuf, csem, rs_s, rs_r, ag_s, ag_r, agc_s, agc_r, agl,
                 sum1, cbuf1, rbuf1, csem1, rs_s1, rs_r1, ag_s1, ag_r1, agc_s1, agc_r1, agl1):
    place = Place()
    me, core = place.me, place.core
    entry_barrier(me)

    def to_partner1(q):
        return rcopy(w_ref.at[:, lanes(2 * place.chip(q) + 1 - core)], cbuf1.at[q], csem1.at[0, q], csem1.at[1, q],
                     place.partner)

    red1 = Reduce(place, lambda q, k: sum1.at[q, pl.ds(128 * k, 128)],
                  lambda s, q, k: rbuf1.at[k, land_slot(s, q, k)], rs_s1, rs_r1)
    ag1 = Spread(place, lambda p, c, k: p_ref.at[pl.ds(128 * k, 128), lanes(2 * p + c)], ag_s1, ag_r1, agc_s1, agc_r1,
                 lambda k: sum1.at[0, pl.ds(128 * k, 128)], agl1)
    for q in Q_ORDER:
        to_partner1(q).start()

    def begin1():
        for q in Q_ORDER:
            to_partner1(q).wait_recv()
            sum1[q] = w_ref[:, lanes(2 * place.chip(q) + core)] + cbuf1[q]
            for k in range(3):
                if sent_stage(q, k) == 0:
                    red1.copy(q, k).start()

    def end1():
        red1.stage(3)
        for k in range(3):
            ag1.start(k)

    also = {0: begin1, 3: lambda: red1.stage(1), 5: lambda: red1.stage(2), 7: end1}

    def to_partner(q):
        return rcopy(part.at[1, q], cbuf.at[q], csem.at[0, q], csem.at[1, q], place.partner)

    def cols(k):
        return pl.ds(*COLS[k])

    red = Reduce(place, lambda q, k: part.at[0, q, :, cols(k)],
                 lambda s, q, k: rbuf.at[k, land_slot(s, q, k), :, pl.ds(0, COLS[k][1])], rs_s, rs_r)
    ag = Spread(place, lambda p, c, k: o_ref.at[pl.ds(pl.multiple_of((2 * p + c) * 128, 128), 128), cols(k)],
                ag_s, ag_r, agc_s, agc_r, lambda k: part.at[0, 0, :, cols(k)], agl)

    def core_sum(q):
        to_partner(q).wait_recv()

        @pl.loop(0, 8)
        def _(n):
            at = pl.ds(pl.multiple_of(n * 256, 256), 256)
            part[0, q, :, at] = part[0, q, :, at] + cbuf[q, :, at]

        for k in range(3):
            if sent_stage(q, k) == 0:
                red.copy(q, k).start()

    for i, q in enumerate(Q_ORDER):
        p = place.chip(q)

        @pl.loop(0, 8)
        def _(n):
            at = pl.ds(pl.multiple_of(n * 256, 256), 256)
            xt[:, at] = jnp.transpose(x_ref[at, pl.ds(pl.multiple_of(p * 256, 256), 256)])

        @pl.loop(0, 8)
        def _(n):
            at = pl.ds(pl.multiple_of(n * 256, 256), 256)
            out = jnp.dot(xt[...], d_ref[:, at], preferred_element_type=jnp.float32)
            part[core, q, :, at] = out[:128]
            part[1 - core, q, :, at] = out[128:]

        to_partner(q).start()
        if i in also:
            also[i]()
        if i > 0:
            core_sum(Q_ORDER[i - 1])
    core_sum(0)
    ag1.run((0,))
    red.stage(1)
    ag1.run((1,))
    red.stage(2)
    ag1.run((2,))
    red.stage(3)
    for k in range(3):
        ag.start(k)
    ag.run()
    ag1.finish()
    ag.finish()
    for q in range(8):
        to_partner(q).wait_send()
        to_partner1(q).wait_send()
    red.drain()
    red1.drain()


def wgrad(x, d, w, cid):
    vm = pl.BlockSpec(memory_space=pltpu.VMEM)
    hbm = pl.BlockSpec(memory_space=pl.ANY)
    dma = pltpu.SemaphoreType.DMA
    sems = [dma((2, 8)), dma((3, 8)), dma((3, 24)), dma((3, 24)), dma((3, 8)), dma((3, 8)), dma((3, 8)), dma((3,))]
    f32 = jnp.float32
    return pl.pallas_call(
        wgrad_kernel,
        out_shape=(jax.ShapeDtypeStruct((DIM, DIM), f32), jax.ShapeDtypeStruct((384, DIM), f32)),
        in_specs=[vm, vm, vm], out_specs=(hbm, hbm),
        scratch_shapes=[pltpu.VMEM((256, 2 * ROWS), jnp.bfloat16), pltpu.VMEM((2, 8, 128, DIM), f32),
                        pltpu.VMEM((8, 128, DIM), f32), pltpu.VMEM((3, 7, 128, 768), f32)] + sems
                       + [pltpu.VMEM((8, 384, 128), f32), pltpu.VMEM((8, 384, 128), f32),
                          pltpu.VMEM((3, 7, 128, 128), f32)] + sems,
        compiler_params=pltpu.CompilerParams(collective_id=cid, has_side_effects=True, vmem_limit_bytes=VMEM_LIMIT),
        cost_estimate=pl.CostEstimate(flops=100_000_000_000, bytes_accessed=60_000_000, transcendentals=0),
        name='wgrad')(x, d, w)


def pad_rows(*rows):
    x = jnp.concatenate(rows, axis=0)
    return jnp.pad(x, ((0, 8 - x.shape[0]), (0, 0)))


def layer_forward(x_in, weight, gain_vec, bias_vec, cid):
    pre_act = jnp.einsum('vnk,kd->vnd', x_in, weight, preferred_element_type=jnp.float32)
    moments = small_sum(pad_rows(jnp.sum(pre_act, axis=1), jnp.sum(pre_act * pre_act, axis=1)), cid)
    col_mean = moments[0:2] / ALL_ROWS
    col_var = moments[2:4] / ALL_ROWS - col_mean * col_mean
    inv_std = lax.rsqrt(col_var + BN_EPS)[:, None, :]
    normed = (pre_act - col_mean[:, None, :]) * inv_std
    act_val = gain_vec * normed + bias_vec
    return jnp.maximum(act_val, 0.0).astype(jnp.bfloat16), normed, act_val, inv_std


def layer_backward(d_out, normed, act_val, inv_std, gain_vec, cid, extra=None):
    d_act = jnp.where(act_val > 0.0, d_out, 0.0)
    rows = [jnp.sum(d_act, axis=1), jnp.sum(d_act * normed, axis=1)]
    if extra is not None:
        rows.append(extra)
    stat_sums = small_sum(pad_rows(*rows), cid)
    mean_d = (stat_sums[0:2] / ALL_ROWS)[:, None, :]
    mean_dn = (stat_sums[2:4] / ALL_ROWS)[:, None, :]
    d_pre = inv_std * gain_vec * (d_act - mean_d - normed * mean_dn)
    return d_pre.astype(jnp.bfloat16), stat_sums[2] + stat_sums[3], stat_sums[0] + stat_sums[1], stat_sums


def solution(mesh):
    def local_step(h_a, h_b, w_one, w_two, w_three, gain_one, bias_one, gain_two, bias_two):
        view_feats = jnp.stack([h_a, h_b])
        hidden_one, normed_one, act_one, inv_one = layer_forward(view_feats, w_one, gain_one, bias_one, 0)
        hidden_two, normed_two, act_two, inv_two = layer_forward(hidden_one, w_two, gain_two, bias_two, 1)
        z_views = jnp.einsum('vnk,kd->vnd', hidden_two, w_three, preferred_element_type=jnp.float32).astype(jnp.bfloat16)
        z_diff = z_views[0].astype(jnp.float32) - z_views[1].astype(jnp.float32)
        stats = pad_rows(jnp.sum(z_views, axis=1, dtype=jnp.float32), jnp.sum(z_diff * z_diff, axis=0)[None])
        pack, tot, loss_part = gram_loss(z_views, stats, 2)
        d_z = dz_call(z_views, pack, tot)
        grad_three = jnp.einsum('vnk,vnd->kd', hidden_two, d_z, preferred_element_type=jnp.float32)
        grad_three = lax.psum(grad_three, 'data')
        d_hidden_two = jnp.einsum('vnd,kd->vnk', d_z, w_three, preferred_element_type=jnp.float32)
        loss_row = jnp.pad(jnp.sum(loss_part, axis=0)[None], ((0, 0), (0, DIM - 128)))
        d_pre_two, gain_grad_two, bias_grad_two, sums = layer_backward(
            d_hidden_two, normed_two, act_two, inv_two, gain_two, 3, loss_row)
        loss_val = INV_WEIGHT * jnp.sum(tot[2]) / ALL_ROWS + jnp.sum(sums[4])
        d_hidden_one = jnp.einsum('vnd,kd->vnk', d_pre_two, w_two, preferred_element_type=jnp.float32)
        d_pre_one, gain_grad_one, bias_grad_one, _ = layer_backward(
            d_hidden_one, normed_one, act_one, inv_one, gain_one, 4)
        grad_one = jnp.einsum('vnf,vnd->fd', view_feats, d_pre_one, preferred_element_type=jnp.float32)
        flat = (2 * ROWS, DIM)
        grad_two, grad_one = wgrad(hidden_one.reshape(flat), d_pre_two.reshape(flat), grad_one, 5)
        return loss_val, grad_one, grad_two, grad_three, gain_grad_one, bias_grad_one, gain_grad_two, bias_grad_two

    row_spec = P('data', None)
    return jax.shard_map(local_step, mesh=mesh,
                         in_specs=(row_spec, row_spec, P(), P(), P(), P(), P(), P(), P()),
                         out_specs=(P(), P(), P(), P(), P(), P(), P(), P()),
                         check_vma=False)
```

```python
import jax
import jax.numpy as jnp
from jax import lax
from jax.experimental import pallas as pl
from jax.experimental.pallas import tpu as pltpu
from jax.sharding import PartitionSpec as P


BN_EPS = 1e-5
STD_EPS = 1e-4
INV_WEIGHT = 2.0
VAR_WEIGHT = 1.0
COV_WEIGHT = 2.0

N_DEV = 16
ROWS = 1024
DIM = 2048
ALL_ROWS = N_DEV * ROWS
MESH = pl.DeviceIdType.MESH
VMEM_LIMIT = 64 * 1024 * 1024 - 128 * 1024

ORDERS = ((0, 1, 2), (1, 2, 0), (2, 0, 1))
Q_ORDER = (7, 6, 5, 3, 4, 2, 1, 0)


def sent_stage(q, k):
    for s, d in enumerate(ORDERS[k]):
        if (q >> d) & 1:
            return s
    return 3


def last_stage(q, k):
    last = -1
    for s, d in enumerate(ORDERS[k]):
        if (q >> d) & 1:
            last = s
    return last


class Place:
    def __init__(self):
        self.me = lax.axis_index('data')
        self.core = self.me % 2
        self.bits = ((self.me // 2) % 2, (self.me // 4) % 2, self.me // 8)
        self.partner = self.me + 1 - 2 * self.core
        self.near = tuple(self.me + (2 << d) - (4 << d) * self.bits[d] for d in range(3))

    def chip(self, q):
        p = 0
        for d in range(3):
            b = self.bits[d]
            p = p + ((1 - b) if (q >> d) & 1 else b) * (1 << d)
        return p


def entry_barrier(me):
    sem = pltpu.get_barrier_semaphore()
    for k in range(1, N_DEV):
        pl.semaphore_signal(sem, inc=1, device_id=((me + k) % N_DEV,), device_id_type=MESH)
    pl.semaphore_wait(sem, N_DEV - 1)


def rcopy(src, dst, ssem, rsem, dev):
    return pltpu.make_async_remote_copy(src_ref=src, dst_ref=dst, send_sem=ssem, recv_sem=rsem,
                                        device_id=(dev,), device_id_type=MESH)


def lanes(i):
    return pl.ds(pl.multiple_of(i * 128, 128), 128)


class SmallSum:
    def __init__(self, me, x_ref, o_ref, slots, sems):
        self.me, self.x, self.o, self.slots, self.sems = me, x_ref, o_ref, slots, sems

    def out_copy(self, k):
        peer = (self.me + k) % N_DEV
        return rcopy(self.x.at[:, lanes(peer)], self.slots.at[self.me], self.sems.at[0, peer],
                     self.sems.at[1, self.me], peer)

    def in_copy(self, k):
        src = (self.me + k) % N_DEV
        return rcopy(self.x.at[:, lanes(src)], self.slots.at[src], self.sems.at[0, src], self.sems.at[1, src], src)

    def out_bcast(self, k):
        peer = (self.me + k) % N_DEV
        mine = self.o.at[:, lanes(self.me)]
        return rcopy(mine, mine, self.sems.at[2, peer], self.sems.at[3, self.me], peer)

    def in_bcast(self, k):
        src = (self.me + k) % N_DEV
        theirs = self.o.at[:, lanes(src)]
        return rcopy(theirs, theirs, self.sems.at[2, src], self.sems.at[3, src], src)

    def start(self):
        for k in range(1, N_DEV):
            self.out_copy(k).start()
        self.slots[self.me] = self.x[:, lanes(self.me)]

    def middle(self):
        for k in range(1, N_DEV):
            self.in_copy(k).wait_recv()
        total = self.slots[0]
        for s in range(1, N_DEV):
            total = total + self.slots[s]
        self.o[:, lanes(self.me)] = total
        for k in range(1, N_DEV):
            self.out_bcast(k).start()

    def finish(self):
        for k in range(1, N_DEV):
            self.in_bcast(k).wait_recv()
        for k in range(1, N_DEV):
            self.out_copy(k).wait_send()
            self.out_bcast(k).wait_send()


SMALL_SCRATCH = [pltpu.VMEM((N_DEV, 8, 128), jnp.float32), pltpu.SemaphoreType.DMA((4, N_DEV))]


def small_sum_kernel(x_ref, o_ref, slots, sems):
    me = lax.axis_index('data')
    entry_barrier(me)
    s = SmallSum(me, x_ref, o_ref, slots, sems)
    s.start()
    s.middle()
    s.finish()


def small_sum(x, cid):
    vm = pl.BlockSpec(memory_space=pltpu.VMEM)
    return pl.pallas_call(
        small_sum_kernel, out_shape=jax.ShapeDtypeStruct((8, DIM), jnp.float32),
        in_specs=[vm], out_specs=vm, scratch_shapes=SMALL_SCRATCH,
        compiler_params=pltpu.CompilerParams(collective_id=cid, has_side_effects=True),
        cost_estimate=pl.CostEstimate(flops=8_000_000, bytes_accessed=131072, transcendentals=0),
        name='small_sum')(x)


class Reduce:
    def __init__(self, place, own, land, ssem, rsem):
        self.place, self.own, self.land, self.ssem, self.rsem = place, own, land, ssem, rsem

    def copy(self, q, k):
        s = sent_stage(q, k)
        d = ORDERS[k][s]
        dst = q & ~(1 << d)
        return rcopy(self.own(q, k), self.land(s, dst, k), self.ssem.at[k, q], self.rsem.at[k, 8 * s + dst],
                     self.place.near[d])

    def arrive(self, q, k, s):
        self.copy(q | (1 << ORDERS[k][s]), k).wait_recv()
        own = self.own(q, k)
        own[...] = own[...] + self.land(s, q, k)[...]

    def stage(self, stage):
        for q in Q_ORDER:
            for k in range(3):
                if sent_stage(q, k) == stage:
                    for s in range(stage):
                        self.arrive(q, k, s)
                    if stage < 3:
                        self.copy(q, k).start()

    def drain(self):
        for k in range(3):
            for q in range(1, 8):
                self.copy(q, k).wait_send()


class Spread:
    def __init__(self, place, piece, ssem, rsem, csend, crecv, mine=None, lsem=None):
        self.place, self.piece, self.mine, self.lsem = place, piece, mine, lsem
        self.ssem, self.rsem, self.csend, self.crecv = ssem, rsem, csend, crecv

    def source(self, q, k):
        if q == 0 and self.mine is not None:
            return self.mine(k)
        return self.piece(self.place.chip(q), self.place.core, k)

    def copy(self, q, k, u):
        d = ORDERS[k][u]
        ref = self.piece(self.place.chip(q), self.place.core, k)
        return rcopy(self.source(q, k), ref, self.ssem.at[k, 3 * q + u], self.rsem.at[k, q | (1 << d)],
                     self.place.near[d])

    def to_partner(self, q, k):
        ref = self.piece(self.place.chip(q), self.place.core, k)
        return rcopy(self.source(q, k), ref, self.csend.at[k, q], self.crecv.at[k, q], self.place.partner)

    def keep(self, k):
        ref = self.piece(self.place.chip(0), self.place.core, k)
        return pltpu.make_async_copy(self.mine(k), ref, self.lsem.at[k])

    def from_partner(self, q, k):
        ref = self.piece(self.place.chip(q), 1 - self.place.core, k)
        return rcopy(ref, ref, self.csend.at[k, q], self.crecv.at[k, q], self.place.partner)

    def start(self, k):
        for u in range(3):
            self.copy(0, k, u).start()
        self.to_partner(0, k).start()
        if self.mine is not None:
            self.keep(k).start()

    def run(self, stages=(0, 1, 2)):
        for stage in stages:
            for q in range(1, 8):
                for k in range(3):
                    if last_stage(q, k) != stage:
                        continue
                    d = ORDERS[k][stage]
                    ref = self.piece(self.place.chip(q), self.place.core, k)
                    rcopy(ref, ref, self.ssem.at[k, 3 * q], self.rsem.at[k, q], self.place.near[d]).wait_recv()
                    for u in range(stage + 1, 3):
                        self.copy(q, k, u).start()
                    self.to_partner(q, k).start()

    def finish(self):
        for q in range(8):
            for k in range(3):
                self.from_partner(q, k).wait_recv()
        for k in range(3):
            if self.mine is not None:
                self.keep(k).wait()
        for q in range(8):
            for k in range(3):
                for u in range(last_stage(q, k) + 1, 3):
                    self.copy(q, k, u).wait_send()
                self.to_partner(q, k).wait_send()


def land_slot(s, q, k):
    order = [x for x in range(8) if sent_stage(x, k) > s]
    return (0, 4, 6)[s] + order.index(q)


def gram_kernel(z_ref, st_ref, pack_ref, tot_ref, loss_ref, gbuf, cbuf, rbuf, slots, sems, csem, rs_s, rs_r,
                ag_s, ag_r, agc_s, agc_r):
    place = Place()
    me, core = place.me, place.core
    entry_barrier(me)
    small = SmallSum(me, st_ref, tot_ref, slots, sems)
    small.start()

    def to_partner(q):
        return rcopy(gbuf.at[1, q, pl.ds(0, 9)], cbuf.at[q], csem.at[0, q], csem.at[1, q], place.partner)

    red = Reduce(place, lambda q, k: gbuf.at[0, q, pl.ds(3 * k, 3)],
                 lambda s, q, k: rbuf.at[k, land_slot(s, q, k)], rs_s, rs_r)

    def core_sum(q):
        to_partner(q).wait_recv()
        mine = gbuf.at[0, q, pl.ds(0, 9)]
        mine[...] = mine[...] + cbuf[q]
        for k in range(3):
            if sent_stage(q, k) == 0:
                red.copy(q, k).start()

    for i, q in enumerate(Q_ORDER):
        p = place.chip(q)

        @pl.loop(0, 2)
        def _(v):
            left = z_ref[v, :, pl.ds(pl.multiple_of(p * 256, 256), 256)]

            @pl.loop(0, 5)
            def _(b):
                right = z_ref[v, :, pl.ds(pl.multiple_of(((p + b) % 8) * 256, 256), 256)]
                out = lax.dot_general(left, right, (((0,), (0,)), ((), ())), preferred_element_type=jnp.float32)
                gbuf[core, q, 2 * b, v] = out[:128, :128]
                gbuf[core, q, 2 * b + 1, v] = out[:128, 128:]
                gbuf[1 - core, q, (2 * b + 9) % 10, v] = out[128:, :128]
                gbuf[1 - core, q, 2 * b, v] = out[128:, 128:]

        to_partner(q).start()
        if i == 1:
            small.middle()
        if i > 0:
            core_sum(Q_ORDER[i - 1])
    core_sum(0)
    for s in (1, 2, 3):
        red.stage(s)
    small.finish()

    ag = Spread(place, lambda p, c, k: pack_ref.at[2 * p + c, pl.ds(3 * k, 3)], ag_s, ag_r, agc_s, agc_r)
    eye = lax.broadcasted_iota(jnp.int32, (128, 128), 0) == lax.broadcasted_iota(jnp.int32, (128, 128), 1)
    acc = jnp.zeros((128, 128), jnp.float32)
    mu_rows = [jnp.transpose(jnp.broadcast_to(tot_ref[pl.ds(v, 1), lanes(me)] / ALL_ROWS, (128, 128))) for v in range(2)]
    for j in range(9):
        for v in range(2):
            mu_cols = tot_ref[pl.ds(v, 1), lanes((me + j) % N_DEV)] / ALL_ROWS
            cov = (gbuf[0, 0, j, v] - ALL_ROWS * mu_rows[v] * mu_cols) / (ALL_ROWS - 1)
            grad = (2.0 * COV_WEIGHT) * cov
            if j == 0:
                std = jnp.sqrt(jnp.where(eye, cov, 1.0) + STD_EPS)
                hinge = (std < 1.0).astype(jnp.float32)
                acc = acc + jnp.where(eye, VAR_WEIGHT * jnp.maximum(1.0 - std, 0.0), COV_WEIGHT * cov * cov)
                grad = jnp.where(eye, -VAR_WEIGHT * hinge / (2.0 * std), grad)
            else:
                acc = acc + (COV_WEIGHT * (2.0 if j < 8 else 1.0)) * cov * cov
            pack_ref[me, j, v] = grad.astype(jnp.bfloat16)
        if j % 3 == 2:
            ag.start(j // 3)
    part = acc[0:8]
    for r in range(1, 16):
        part = part + acc[8 * r:8 * r + 8]
    loss_ref[...] = part
    ag.run()
    ag.finish()
    for q in range(8):
        to_partner(q).wait_send()
    red.drain()


def gram_loss(z, stats, cid):
    vm = pl.BlockSpec(memory_space=pltpu.VMEM)
    dma = pltpu.SemaphoreType.DMA
    return pl.pallas_call(
        gram_kernel,
        out_shape=(jax.ShapeDtypeStruct((N_DEV, 9, 2, 128, 128), jnp.bfloat16),
                   jax.ShapeDtypeStruct((8, DIM), jnp.float32),
                   jax.ShapeDtypeStruct((8, 128), jnp.float32)),
        in_specs=[vm, vm], out_specs=(vm, vm, vm),
        scratch_shapes=[pltpu.VMEM((2, 8, 10, 2, 128, 128), jnp.float32),
                        pltpu.VMEM((8, 9, 2, 128, 128), jnp.float32),
                        pltpu.VMEM((3, 7, 3, 2, 128, 128), jnp.float32)] + SMALL_SCRATCH
                       + [dma((2, 8)), dma((3, 8)), dma((3, 24)), dma((3, 24)), dma((3, 8)), dma((3, 8)), dma((3, 8))],
        compiler_params=pltpu.CompilerParams(collective_id=cid, has_side_effects=True, vmem_limit_bytes=VMEM_LIMIT),
        cost_estimate=pl.CostEstimate(flops=60_000_000_000, bytes_accessed=20_000_000, transcendentals=0),
        name='gram_loss')(z, stats)


def dz_kernel(z_ref, pack_ref, tot_ref, o_ref, gcol):
    v, t = pl.program_id(0), pl.program_id(1)
    for h in range(2):
        c = 2 * t + h
        col = pl.ds(128 * h, 128)
        for d in range(16):
            r = (c + 16 - d) % 16
            rows = pl.ds(pl.multiple_of(r * 128, 128), 128)
            if d <= 8:
                gcol[rows, col] = pack_ref[r, d, v]
            else:
                gcol[rows, col] = jnp.transpose(pack_ref[c, 16 - d, v])
    mu = jnp.broadcast_to(tot_ref[pl.ds(v, 1), :] / ALL_ROWS, (16, DIM))
    high = mu.astype(jnp.bfloat16).astype(jnp.float32)
    mid = (mu - high).astype(jnp.bfloat16).astype(jnp.float32)
    low = mu - high - mid
    row = lax.broadcasted_iota(jnp.int32, (16, DIM), 0)
    terms = jnp.where(row == 0, high, jnp.where(row == 1, mid, jnp.where(row == 2, low, 0.0))).astype(jnp.bfloat16)
    mean = jnp.sum(jnp.dot(terms, gcol[...], preferred_element_type=jnp.float32), axis=0, keepdims=True)
    sign = (1 - 2 * v).astype(jnp.float32) * (2.0 * INV_WEIGHT / ALL_ROWS)
    cols = pl.ds(pl.multiple_of(t * 256, 256), 256)

    @pl.loop(0, 4)
    def _(m):
        rows = pl.ds(pl.multiple_of(m * 256, 256), 256)
        acc = jnp.dot(z_ref[v, rows, :], gcol[...], preferred_element_type=jnp.float32)
        diff = z_ref[0, rows, cols].astype(jnp.float32) - z_ref[1, rows, cols].astype(jnp.float32)
        o_ref[0, rows, :] = ((2.0 / (ALL_ROWS - 1)) * (acc - mean) + sign * diff).astype(jnp.bfloat16)


def dz_call(z, pack, tot):
    full = lambda shape: pl.BlockSpec(shape, lambda v, t: (0,) * len(shape), pipeline_mode=pl.Buffered(1))
    return pl.pallas_call(
        dz_kernel, grid=(2, 8), out_shape=jax.ShapeDtypeStruct((2, ROWS, DIM), jnp.bfloat16),
        in_specs=[full((2, ROWS, DIM)), full((N_DEV, 9, 2, 128, 128)), full((8, DIM))],
        out_specs=pl.BlockSpec((1, ROWS, 256), lambda v, t: (v, 0, t)),
        scratch_shapes=[pltpu.VMEM((DIM, 256), jnp.bfloat16)],
        compiler_params=pltpu.CompilerParams(vmem_limit_bytes=40 * 1024 * 1024,
                                             dimension_semantics=('arbitrary', 'arbitrary')),
        cost_estimate=pl.CostEstimate(flops=2 * 2 * ROWS * DIM * DIM, bytes_accessed=27_000_000, transcendentals=0),
        name='dz')(z, pack, tot)


def wsum_kernel(w_ref, p_ref, sum1, cbuf1, rbuf1, csem1, rs_s1, rs_r1, ag_s1, ag_r1, agc_s1, agc_r1, agl1):
    place = Place()
    core = place.core
    entry_barrier(place.me)

    def to_partner(q):
        return rcopy(w_ref.at[:, lanes(2 * place.chip(q) + 1 - core)], cbuf1.at[q], csem1.at[0, q], csem1.at[1, q],
                     place.partner)

    red = Reduce(place, lambda q, k: sum1.at[q, pl.ds(128 * k, 128)],
                 lambda s, q, k: rbuf1.at[k, land_slot(s, q, k)], rs_s1, rs_r1)
    ag = Spread(place, lambda p, c, k: p_ref.at[pl.ds(128 * k, 128), lanes(2 * p + c)], ag_s1, ag_r1, agc_s1, agc_r1,
                lambda k: sum1.at[0, pl.ds(128 * k, 128)], agl1)
    for q in Q_ORDER:
        to_partner(q).start()
    for q in Q_ORDER:
        to_partner(q).wait_recv()
        sum1[q] = w_ref[:, lanes(2 * place.chip(q) + core)] + cbuf1[q]
        for k in range(3):
            if sent_stage(q, k) == 0:
                red.copy(q, k).start()
    for s in (1, 2, 3):
        red.stage(s)
    for k in range(3):
        ag.start(k)
    ag.run()
    ag.finish()
    for q in range(8):
        to_partner(q).wait_send()
    red.drain()


def wsum(w, cid):
    vm = pl.BlockSpec(memory_space=pltpu.VMEM)
    dma = pltpu.SemaphoreType.DMA
    f32 = jnp.float32
    return pl.pallas_call(
        wsum_kernel, out_shape=jax.ShapeDtypeStruct((384, DIM), f32), in_specs=[vm], out_specs=vm,
        scratch_shapes=[pltpu.VMEM((8, 384, 128), f32), pltpu.VMEM((8, 384, 128), f32), pltpu.VMEM((3, 7, 128, 128), f32),
                        dma((2, 8)), dma((3, 8)), dma((3, 24)), dma((3, 24)), dma((3, 8)), dma((3, 8)), dma((3, 8)),
                        dma((3,))],
        compiler_params=pltpu.CompilerParams(collective_id=cid, has_side_effects=True),
        cost_estimate=pl.CostEstimate(flops=20_000_000_000, bytes_accessed=6_000_000, transcendentals=0),
        name='wsum')(w)


COLS = ((0, 640), (640, 640), (1280, 768))
TILE = 256


def tile_at(n):
    return pl.ds(pl.multiple_of(n * TILE, TILE), TILE)


def layer_kernel(x_hbm, d_hbm, w_hbm, pre_hbm, vec_ref, init_ref, shard_ref, tot_ref, act_hbm,
                 x_ref, d_ref, w_ref, tile, st, xt, part, cbuf, rbuf, xsem, dwsem, tsem, slots, sems, csem, rs_s, rs_r):
    place = Place()
    me, core = place.me, place.core
    load_d = pltpu.make_async_copy(d_hbm, d_ref, dwsem.at[0])
    load_w = pltpu.make_async_copy(w_hbm, w_ref, dwsem.at[1])

    def load_x(q):
        at = tile_at(place.chip(q))
        return pltpu.make_async_copy(x_hbm.at[:, at], x_ref.at[:, at], xsem.at[q])

    def load_tile(m):
        return pltpu.make_async_copy(pre_hbm.at[pl.ds(m * TILE, TILE)], tile.at[m % 2], tsem.at[0, m % 2])

    def save_tile(m):
        return pltpu.make_async_copy(tile.at[m % 2], act_hbm.at[pl.ds(m * TILE, TILE)], tsem.at[1, m % 2])

    load_x(Q_ORDER[0]).start()
    load_d.start()
    for q in Q_ORDER[1:]:
        load_x(q).start()
    load_w.start()
    load_tile(0).start()
    st[...] = init_ref[...]
    entry_barrier(me)
    small = SmallSum(me, st, tot_ref, slots, sems)

    def to_partner(q):
        return rcopy(part.at[1, q], cbuf.at[q], csem.at[0, q], csem.at[1, q], place.partner)

    def cols(k):
        return pl.ds(*COLS[k])

    red = Reduce(place, lambda q, k: part.at[0, q, :, cols(k)],
                 lambda s, q, k: rbuf.at[k, land_slot(s, q, k), :, pl.ds(0, COLS[k][1])], rs_s, rs_r)

    def core_sum(q):
        to_partner(q).wait_recv()

        @pl.loop(0, 8)
        def _(n):
            at = tile_at(n)
            part[0, q, :, at] = part[0, q, :, at] + cbuf[q, :, at]

        for k in range(3):
            if sent_stage(q, k) == 0:
                red.copy(q, k).start()

    def chunk(m):
        v, s = m // 4, m % 2
        if m > 0:
            save_tile(m - 1).wait()
        if m < 7:
            load_tile(m + 1).start()
        load_tile(m).wait()
        rows = pl.ds(m * TILE, TILE)

        @pl.loop(0, 8)
        def _(n):
            at = tile_at(n)
            grad = lax.dot_general(d_ref[rows, :], w_ref[at, :], (((1,), (1,)), ((), ())),
                                   preferred_element_type=jnp.float32)
            normed = (tile[s, :, at] - vec_ref[pl.ds(v, 1), at]) * vec_ref[pl.ds(2 + v, 1), at]
            act = vec_ref[pl.ds(4, 1), at] * normed + vec_ref[pl.ds(5, 1), at]
            grad = jnp.where(act > 0.0, grad, 0.0)
            tile[s, :, at] = grad
            st[pl.ds(v, 1), at] = st[pl.ds(v, 1), at] + jnp.sum(grad, axis=0, keepdims=True)
            st[pl.ds(2 + v, 1), at] = st[pl.ds(2 + v, 1), at] + jnp.sum(grad * normed, axis=0, keepdims=True)

        save_tile(m).start()

    for i, q in enumerate(Q_ORDER):
        p = place.chip(q)
        load_x(q).wait()

        @pl.loop(0, 8)
        def _(n):
            at = tile_at(n)
            xt[:, at] = jnp.transpose(x_ref[at, tile_at(p)])

        if i == 0:
            load_d.wait()

        @pl.loop(0, 8)
        def _(n):
            at = tile_at(n)
            out = jnp.dot(xt[...], d_ref[:, at], preferred_element_type=jnp.float32)
            part[core, q, :, at] = out[:128]
            part[1 - core, q, :, at] = out[128:]

        to_partner(q).start()
        if i > 0:
            core_sum(Q_ORDER[i - 1])
    load_w.wait()
    chunk(0)
    core_sum(0)
    for m in range(1, 5):
        chunk(m)
    red.stage(1)
    for m in range(5, 8):
        chunk(m)
    small.start()
    red.stage(2)
    small.middle()
    red.stage(3)
    shard_ref[...] = part[0, 0]
    small.finish()
    save_tile(7).wait()
    for q in range(8):
        to_partner(q).wait_send()
    red.drain()


def layer_call(x, d, w, pre, vecs, init, cid):
    vm = pl.BlockSpec(memory_space=pltpu.VMEM)
    hbm = pl.BlockSpec(memory_space=pl.ANY)
    dma = pltpu.SemaphoreType.DMA
    f32, bf16 = jnp.float32, jnp.bfloat16
    rows = 2 * ROWS
    return pl.pallas_call(
        layer_kernel,
        out_shape=(jax.ShapeDtypeStruct((128, DIM), f32), jax.ShapeDtypeStruct((8, DIM), f32),
                   jax.ShapeDtypeStruct((rows, DIM), f32)),
        in_specs=[hbm, hbm, hbm, hbm, vm, vm], out_specs=(vm, vm, hbm),
        scratch_shapes=[pltpu.VMEM((rows, DIM), bf16), pltpu.VMEM((rows, DIM), bf16), pltpu.VMEM((DIM, DIM), bf16),
                        pltpu.VMEM((2, TILE, DIM), f32), pltpu.VMEM((8, DIM), f32), pltpu.VMEM((TILE, rows), bf16),
                        pltpu.VMEM((2, 8, 128, DIM), f32), pltpu.VMEM((8, 128, DIM), f32),
                        pltpu.VMEM((3, 7, 128, 768), f32), dma((8,)), dma((2,)), dma((2, 2))] + SMALL_SCRATCH
                       + [dma((2, 8)), dma((3, 8)), dma((3, 24))],
        compiler_params=pltpu.CompilerParams(collective_id=cid, has_side_effects=True, vmem_limit_bytes=VMEM_LIMIT),
        cost_estimate=pl.CostEstimate(flops=50_000_000_000, bytes_accessed=60_000_000, transcendentals=0),
        name='layer_back')(x, d, w, pre, vecs, init)


def pad_rows(*rows):
    x = jnp.concatenate(rows, axis=0)
    return jnp.pad(x, ((0, 8 - x.shape[0]), (0, 0)))


def layer_forward(x_in, weight, gain_vec, bias_vec, cid):
    pre_act = jnp.einsum('vnk,kd->vnd', x_in, weight, preferred_element_type=jnp.float32)
    moments = small_sum(pad_rows(jnp.sum(pre_act, axis=1), jnp.sum(pre_act * pre_act, axis=1)), cid)
    col_mean = moments[0:2] / ALL_ROWS
    col_var = moments[2:4] / ALL_ROWS - col_mean * col_mean
    inv_std = lax.rsqrt(col_var + BN_EPS)
    normed = (pre_act - col_mean[:, None, :]) * inv_std[:, None, :]
    act_val = gain_vec * normed + bias_vec
    vecs = pad_rows(col_mean, inv_std, gain_vec[None], bias_vec[None])
    return jnp.maximum(act_val, 0.0).astype(jnp.bfloat16), pre_act, normed, inv_std, vecs


def layer_backward(x, d, w, saved, gain_vec, init, cid):
    pre_act, normed, inv_std, vecs = saved
    flat = (2 * ROWS, DIM)
    shard, sums, d_act = layer_call(x.reshape(flat), d.reshape(flat), w, pre_act.reshape(flat), vecs, init, cid)
    mean_d = (sums[0:2] / ALL_ROWS)[:, None, :]
    mean_dn = (sums[2:4] / ALL_ROWS)[:, None, :]
    d_pre = inv_std[:, None, :] * gain_vec * (d_act.reshape(2, ROWS, DIM) - mean_d - normed * mean_dn)
    grad_w = lax.all_gather(shard, 'data', axis=0, tiled=True)
    return d_pre.astype(jnp.bfloat16), grad_w, sums[2] + sums[3], sums[0] + sums[1], sums


def solution(mesh):
    def local_step(h_a, h_b, w_one, w_two, w_three, gain_one, bias_one, gain_two, bias_two):
        view_feats = jnp.stack([h_a, h_b])
        hidden_one, *saved_one = layer_forward(view_feats, w_one, gain_one, bias_one, 0)
        hidden_two, *saved_two = layer_forward(hidden_one, w_two, gain_two, bias_two, 1)
        z_views = jnp.einsum('vnk,kd->vnd', hidden_two, w_three, preferred_element_type=jnp.float32).astype(jnp.bfloat16)
        z_diff = z_views[0].astype(jnp.float32) - z_views[1].astype(jnp.float32)
        stats = pad_rows(jnp.sum(z_views, axis=1, dtype=jnp.float32), jnp.sum(z_diff * z_diff, axis=0)[None])
        pack, tot, loss_part = gram_loss(z_views, stats, 2)
        d_z = dz_call(z_views, pack, tot)
        loss_row = jnp.pad(jnp.sum(loss_part, axis=0)[None], ((4, 3), (0, DIM - 128)))
        d_pre_two, grad_three, gain_grad_two, bias_grad_two, sums = layer_backward(
            hidden_two, d_z, w_three, saved_two, gain_two, loss_row, 3)
        loss_val = INV_WEIGHT * jnp.sum(tot[2]) / ALL_ROWS + jnp.sum(sums[4])
        d_pre_one, grad_two, gain_grad_one, bias_grad_one, _ = layer_backward(
            hidden_one, d_pre_two, w_two, saved_one, gain_one, jnp.zeros((8, DIM), jnp.float32), 4)
        grad_one = wsum(jnp.einsum('vnf,vnd->fd', view_feats, d_pre_one, preferred_element_type=jnp.float32), 5)
        return loss_val, grad_one, grad_two, grad_three, gain_grad_one, bias_grad_one, gain_grad_two, bias_grad_two

    row_spec = P('data', None)
    return jax.shard_map(local_step, mesh=mesh,
                         in_specs=(row_spec, row_spec, P(), P(), P(), P(), P(), P(), P()),
                         out_specs=(P(), P(), P(), P(), P(), P(), P(), P()),
                         check_vma=False)
```

```python
import jax
import jax.numpy as jnp
from jax import lax
from jax.experimental import pallas as pl
from jax.experimental.pallas import tpu as pltpu
from jax.sharding import PartitionSpec as P


BN_EPS = 1e-5
STD_EPS = 1e-4
INV_WEIGHT = 2.0
VAR_WEIGHT = 1.0
COV_WEIGHT = 2.0

N_DEV = 16
ROWS = 1024
DIM = 2048
ALL_ROWS = N_DEV * ROWS
MESH = pl.DeviceIdType.MESH
VMEM_LIMIT = 64 * 1024 * 1024 - 128 * 1024

ORDERS = ((0, 1, 2), (1, 2, 0), (2, 0, 1))
Q_ORDER = (7, 6, 5, 3, 4, 2, 1, 0)


def sent_stage(q, k):
    for s, d in enumerate(ORDERS[k]):
        if (q >> d) & 1:
            return s
    return 3


def last_stage(q, k):
    last = -1
    for s, d in enumerate(ORDERS[k]):
        if (q >> d) & 1:
            last = s
    return last


class Place:
    def __init__(self):
        self.me = lax.axis_index('data')
        self.core = self.me % 2
        self.bits = ((self.me // 2) % 2, (self.me // 4) % 2, self.me // 8)
        self.partner = self.me + 1 - 2 * self.core
        self.near = tuple(self.me + (2 << d) - (4 << d) * self.bits[d] for d in range(3))

    def chip(self, q):
        p = 0
        for d in range(3):
            b = self.bits[d]
            p = p + ((1 - b) if (q >> d) & 1 else b) * (1 << d)
        return p


def entry_barrier(me):
    sem = pltpu.get_barrier_semaphore()
    for k in range(1, N_DEV):
        pl.semaphore_signal(sem, inc=1, device_id=((me + k) % N_DEV,), device_id_type=MESH)
    pl.semaphore_wait(sem, N_DEV - 1)


def rcopy(src, dst, ssem, rsem, dev):
    return pltpu.make_async_remote_copy(src_ref=src, dst_ref=dst, send_sem=ssem, recv_sem=rsem,
                                        device_id=(dev,), device_id_type=MESH)


def lanes(i):
    return pl.ds(pl.multiple_of(i * 128, 128), 128)


class SmallSum:
    def __init__(self, me, x_ref, o_ref, slots, sems):
        self.me, self.x, self.o, self.slots, self.sems = me, x_ref, o_ref, slots, sems

    def out_copy(self, k):
        peer = (self.me + k) % N_DEV
        return rcopy(self.x.at[:, lanes(peer)], self.slots.at[self.me], self.sems.at[0, peer],
                     self.sems.at[1, self.me], peer)

    def in_copy(self, k):
        src = (self.me + k) % N_DEV
        return rcopy(self.x.at[:, lanes(src)], self.slots.at[src], self.sems.at[0, src], self.sems.at[1, src], src)

    def out_bcast(self, k):
        peer = (self.me + k) % N_DEV
        mine = self.o.at[:, lanes(self.me)]
        return rcopy(mine, mine, self.sems.at[2, peer], self.sems.at[3, self.me], peer)

    def in_bcast(self, k):
        src = (self.me + k) % N_DEV
        theirs = self.o.at[:, lanes(src)]
        return rcopy(theirs, theirs, self.sems.at[2, src], self.sems.at[3, src], src)

    def start(self):
        for k in range(1, N_DEV):
            self.out_copy(k).start()
        self.slots[self.me] = self.x[:, lanes(self.me)]

    def middle(self):
        for k in range(1, N_DEV):
            self.in_copy(k).wait_recv()
        total = self.slots[0]
        for s in range(1, N_DEV):
            total = total + self.slots[s]
        self.o[:, lanes(self.me)] = total
        for k in range(1, N_DEV):
            self.out_bcast(k).start()

    def finish(self):
        for k in range(1, N_DEV):
            self.in_bcast(k).wait_recv()
        for k in range(1, N_DEV):
            self.out_copy(k).wait_send()
            self.out_bcast(k).wait_send()


SMALL_SCRATCH = [pltpu.VMEM((N_DEV, 8, 128), jnp.float32), pltpu.SemaphoreType.DMA((4, N_DEV))]


def small_sum_kernel(x_ref, o_ref, slots, sems):
    me = lax.axis_index('data')
    entry_barrier(me)
    s = SmallSum(me, x_ref, o_ref, slots, sems)
    s.start()
    s.middle()
    s.finish()


def small_sum(x, cid):
    vm = pl.BlockSpec(memory_space=pltpu.VMEM)
    return pl.pallas_call(
        small_sum_kernel, out_shape=jax.ShapeDtypeStruct((8, DIM), jnp.float32),
        in_specs=[vm], out_specs=vm, scratch_shapes=SMALL_SCRATCH,
        compiler_params=pltpu.CompilerParams(collective_id=cid, has_side_effects=True),
        cost_estimate=pl.CostEstimate(flops=8_000_000, bytes_accessed=131072, transcendentals=0),
        name='small_sum')(x)


class Reduce:
    def __init__(self, place, own, land, ssem, rsem):
        self.place, self.own, self.land, self.ssem, self.rsem = place, own, land, ssem, rsem

    def copy(self, q, k):
        s = sent_stage(q, k)
        d = ORDERS[k][s]
        dst = q & ~(1 << d)
        return rcopy(self.own(q, k), self.land(s, dst, k), self.ssem.at[k, q], self.rsem.at[k, 8 * s + dst],
                     self.place.near[d])

    def arrive(self, q, k, s):
        self.copy(q | (1 << ORDERS[k][s]), k).wait_recv()
        own = self.own(q, k)
        own[...] = own[...] + self.land(s, q, k)[...]

    def stage(self, stage):
        for q in Q_ORDER:
            for k in range(3):
                if sent_stage(q, k) == stage:
                    for s in range(stage):
                        self.arrive(q, k, s)
                    if stage < 3:
                        self.copy(q, k).start()

    def drain(self):
        for k in range(3):
            for q in range(1, 8):
                self.copy(q, k).wait_send()


class Spread:
    def __init__(self, place, piece, ssem, rsem, csend, crecv, mine=None, lsem=None):
        self.place, self.piece, self.mine, self.lsem = place, piece, mine, lsem
        self.ssem, self.rsem, self.csend, self.crecv = ssem, rsem, csend, crecv

    def source(self, q, k):
        if q == 0 and self.mine is not None:
            return self.mine(k)
        return self.piece(self.place.chip(q), self.place.core, k)

    def copy(self, q, k, u):
        d = ORDERS[k][u]
        ref = self.piece(self.place.chip(q), self.place.core, k)
        return rcopy(self.source(q, k), ref, self.ssem.at[k, 3 * q + u], self.rsem.at[k, q | (1 << d)],
                     self.place.near[d])

    def to_partner(self, q, k):
        ref = self.piece(self.place.chip(q), self.place.core, k)
        return rcopy(self.source(q, k), ref, self.csend.at[k, q], self.crecv.at[k, q], self.place.partner)

    def keep(self, k):
        ref = self.piece(self.place.chip(0), self.place.core, k)
        return pltpu.make_async_copy(self.mine(k), ref, self.lsem.at[k])

    def from_partner(self, q, k):
        ref = self.piece(self.place.chip(q), 1 - self.place.core, k)
        return rcopy(ref, ref, self.csend.at[k, q], self.crecv.at[k, q], self.place.partner)

    def start(self, k):
        for u in range(3):
            self.copy(0, k, u).start()
        self.to_partner(0, k).start()
        if self.mine is not None:
            self.keep(k).start()

    def run(self, stages=(0, 1, 2)):
        for stage in stages:
            for q in range(1, 8):
                for k in range(3):
                    if last_stage(q, k) != stage:
                        continue
                    d = ORDERS[k][stage]
                    ref = self.piece(self.place.chip(q), self.place.core, k)
                    rcopy(ref, ref, self.ssem.at[k, 3 * q], self.rsem.at[k, q], self.place.near[d]).wait_recv()
                    for u in range(stage + 1, 3):
                        self.copy(q, k, u).start()
                    self.to_partner(q, k).start()

    def finish(self):
        for q in range(8):
            for k in range(3):
                self.from_partner(q, k).wait_recv()
        for k in range(3):
            if self.mine is not None:
                self.keep(k).wait()
        for q in range(8):
            for k in range(3):
                for u in range(last_stage(q, k) + 1, 3):
                    self.copy(q, k, u).wait_send()
                self.to_partner(q, k).wait_send()


def land_slot(s, q, k):
    order = [x for x in range(8) if sent_stage(x, k) > s]
    return (0, 4, 6)[s] + order.index(q)


def gram_kernel(z_ref, st_ref, dz_ref, tot_ref, loss_ref, gbuf, cbuf, rbuf, pack_ref, gcol, terms, stage_buf,
                slots, sems, csem, rs_s, rs_r, ag_s, ag_r, agc_s, agc_r, osem):
    place = Place()
    me, core = place.me, place.core
    entry_barrier(me)
    small = SmallSum(me, st_ref, tot_ref, slots, sems)
    small.start()

    def to_partner(q):
        return rcopy(gbuf.at[1, q, :, pl.ds(0, 9)], cbuf.at[q], csem.at[0, q], csem.at[1, q], place.partner)

    red = Reduce(place, lambda q, k: gbuf.at[0, q, :, pl.ds(3 * k, 3)],
                 lambda s, q, k: rbuf.at[k, land_slot(s, q, k)], rs_s, rs_r)

    def core_sum(q):
        to_partner(q).wait_recv()
        mine = gbuf.at[0, q, :, pl.ds(0, 9)]
        mine[...] = mine[...] + cbuf[q]
        for k in range(3):
            if sent_stage(q, k) == 0:
                red.copy(q, k).start()

    for i, q in enumerate(Q_ORDER):
        p = place.chip(q)

        @pl.loop(0, 2)
        def _(v):
            left = z_ref[v, :, pl.ds(pl.multiple_of(p * 256, 256), 256)]

            @pl.loop(0, 5)
            def _(b):
                right = z_ref[v, :, pl.ds(pl.multiple_of(((p + b) % 8) * 256, 256), 256)]
                out = lax.dot_general(left, right, (((0,), (0,)), ((), ())), preferred_element_type=jnp.float32)
                gbuf[core, q, v, 2 * b] = out[:128, :128]
                gbuf[core, q, v, 2 * b + 1] = out[:128, 128:]
                gbuf[1 - core, q, v, (2 * b + 9) % 10] = out[128:, :128]
                gbuf[1 - core, q, v, 2 * b] = out[128:, 128:]

        to_partner(q).start()
        if i == 1:
            small.middle()
        if i > 0:
            core_sum(Q_ORDER[i - 1])
    core_sum(0)
    red.stage(1)
    small.finish()
    red.stage(2)
    red.stage(3)

    def gather(v):
        return Spread(place, lambda p, c, k: pack_ref.at[2 * p + c, v, pl.ds(3 * k, 3)],
                      ag_s.at[v], ag_r.at[v], agc_s.at[v], agc_r.at[v])

    eye = lax.broadcasted_iota(jnp.int32, (128, 128), 0) == lax.broadcasted_iota(jnp.int32, (128, 128), 1)
    acc = jnp.zeros((128, 128), jnp.float32)
    for v in range(2):
        mu_rows = jnp.transpose(jnp.broadcast_to(tot_ref[pl.ds(v, 1), lanes(me)] / ALL_ROWS, (128, 128)))
        for j in range(9):
            mu_cols = tot_ref[pl.ds(v, 1), lanes((me + j) % N_DEV)] / ALL_ROWS
            cov = (gbuf[0, 0, v, j] - ALL_ROWS * mu_rows * mu_cols) / (ALL_ROWS - 1)
            grad = (2.0 * COV_WEIGHT) * cov
            if j == 0:
                std = jnp.sqrt(jnp.where(eye, cov, 1.0) + STD_EPS)
                hinge = (std < 1.0).astype(jnp.float32)
                acc = acc + jnp.where(eye, VAR_WEIGHT * jnp.maximum(1.0 - std, 0.0), COV_WEIGHT * cov * cov)
                grad = jnp.where(eye, -VAR_WEIGHT * hinge / (2.0 * std), grad)
            else:
                acc = acc + (COV_WEIGHT * (2.0 if j < 8 else 1.0)) * cov * cov
            pack_ref[me, v, j] = grad.astype(jnp.bfloat16)
            if j % 3 == 2:
                gather(v).start(j // 3)
    part = acc[0:8]
    for r in range(1, 16):
        part = part + acc[8 * r:8 * r + 8]
    loss_ref[...] = part
    row = lax.broadcasted_iota(jnp.int32, (16, DIM), 0)
    for v in range(2):
        mu = jnp.broadcast_to(tot_ref[pl.ds(v, 1), :] / ALL_ROWS, (16, DIM))
        high = mu.astype(jnp.bfloat16).astype(jnp.float32)
        mid = (mu - high).astype(jnp.bfloat16).astype(jnp.float32)
        low = mu - high - mid
        terms[v] = jnp.where(row == 0, high, jnp.where(row == 1, mid, jnp.where(row == 2, low, 0.0))).astype(jnp.bfloat16)

    def put(v, t):
        cols = pl.ds(pl.multiple_of(t * 256, 256), 256)
        return pltpu.make_async_copy(stage_buf.at[t % 2], dz_ref.at[v, :, cols], osem.at[t % 2])

    def dz_tiles(v, first, last):
        sign = (1 - 2 * v) * (2.0 * INV_WEIGHT / ALL_ROWS)

        @pl.loop(first, last)
        def _(t):
            for h in range(2):
                c = 2 * t + h
                col = pl.ds(128 * h, 128)
                for d in range(16):
                    r = (c + 16 - d) % 16
                    rows = pl.ds(pl.multiple_of(r * 128, 128), 128)
                    if d <= 8:
                        gcol[rows, col] = pack_ref[r, v, d]
                    else:
                        gcol[rows, col] = jnp.transpose(pack_ref[c, v, 16 - d])
            mean = jnp.sum(jnp.dot(terms[v], gcol[...], preferred_element_type=jnp.float32), axis=0, keepdims=True)
            cols = pl.ds(pl.multiple_of(t * 256, 256), 256)

            @pl.when(t >= 2)
            def _():
                put(v, t).wait()

            @pl.loop(0, 4)
            def _(m):
                rows = pl.ds(pl.multiple_of(m * 256, 256), 256)
                acc = jnp.dot(z_ref[v, rows, :], gcol[...], preferred_element_type=jnp.float32)
                diff = z_ref[0, rows, cols].astype(jnp.float32) - z_ref[1, rows, cols].astype(jnp.float32)
                stage_buf[t % 2, rows, :] = ((2.0 / (ALL_ROWS - 1)) * (acc - mean) + sign * diff).astype(jnp.bfloat16)

            put(v, t).start()

    gather(0).run()
    gather(0).finish()
    dz_tiles(0, 0, 2)
    gather(1).run((0,))
    dz_tiles(0, 2, 4)
    gather(1).run((1,))
    dz_tiles(0, 4, 8)
    put(0, 6).wait()
    put(0, 7).wait()
    gather(1).run((2,))
    gather(1).finish()
    dz_tiles(1, 0, 8)
    put(1, 6).wait()
    put(1, 7).wait()
    for q in range(8):
        to_partner(q).wait_send()
    red.drain()


def gram_loss(z, stats, cid):
    vm = pl.BlockSpec(memory_space=pltpu.VMEM)
    dma = pltpu.SemaphoreType.DMA
    f32, bf16 = jnp.float32, jnp.bfloat16
    return pl.pallas_call(
        gram_kernel,
        out_shape=(jax.ShapeDtypeStruct((2, ROWS, DIM), bf16), jax.ShapeDtypeStruct((8, DIM), f32),
                   jax.ShapeDtypeStruct((8, 128), f32)),
        in_specs=[vm, vm], out_specs=(pl.BlockSpec(memory_space=pl.ANY), vm, vm),
        scratch_shapes=[pltpu.VMEM((2, 8, 2, 10, 128, 128), f32), pltpu.VMEM((8, 2, 9, 128, 128), f32),
                        pltpu.VMEM((3, 7, 2, 3, 128, 128), f32), pltpu.VMEM((N_DEV, 2, 9, 128, 128), bf16),
                        pltpu.VMEM((DIM, 256), bf16), pltpu.VMEM((2, 16, DIM), bf16), pltpu.VMEM((2, ROWS, 256), bf16)]
                       + SMALL_SCRATCH + [dma((2, 8)), dma((3, 8)), dma((3, 24)), dma((2, 3, 24)), dma((2, 3, 8)),
                                          dma((2, 3, 8)), dma((2, 3, 8)), dma((2,))],
        compiler_params=pltpu.CompilerParams(collective_id=cid, has_side_effects=True, vmem_limit_bytes=VMEM_LIMIT),
        cost_estimate=pl.CostEstimate(flops=80_000_000_000, bytes_accessed=20_000_000, transcendentals=0),
        name='gram_loss')(z, stats)


def place_kernel(x_ref, o_ref, t_ref):
    o_ref[...] = x_ref[...]
    t_ref[...] = jnp.zeros_like(t_ref)


def place_result(x):
    spec = pl.BlockSpec((256, DIM), lambda i: (i, 0))
    return pl.pallas_call(
        place_kernel, grid=(DIM // 256,),
        out_shape=(jax.ShapeDtypeStruct((DIM, DIM), jnp.float32), jax.ShapeDtypeStruct((8, 128), jnp.float32)),
        in_specs=[spec], out_specs=(spec, pl.BlockSpec((8, 128), lambda i: (0, 0))),
        compiler_params=pltpu.CompilerParams(vmem_limit_bytes=16 * 1024 * 1024),
        cost_estimate=pl.CostEstimate(flops=8_000_000_000, bytes_accessed=33_600_000, transcendentals=0),
        name='place_result')(x)


def wsum_kernel(w_ref, token_ref, p_ref, sum1, cbuf1, rbuf1, csem1, rs_s1, rs_r1, ag_s1, ag_r1, agc_s1, agc_r1, agl1):
    place = Place()
    core = place.core
    entry_barrier(place.me)

    def to_partner(q):
        return rcopy(w_ref.at[:, lanes(2 * place.chip(q) + 1 - core)], cbuf1.at[q], csem1.at[0, q], csem1.at[1, q],
                     place.partner)

    red = Reduce(place, lambda q, k: sum1.at[q, pl.ds(128 * k, 128)],
                 lambda s, q, k: rbuf1.at[k, land_slot(s, q, k)], rs_s1, rs_r1)
    ag = Spread(place, lambda p, c, k: p_ref.at[pl.ds(128 * k, 128), lanes(2 * p + c)], ag_s1, ag_r1, agc_s1, agc_r1,
                lambda k: sum1.at[0, pl.ds(128 * k, 128)], agl1)
    for q in Q_ORDER:
        to_partner(q).start()
    for q in Q_ORDER:
        to_partner(q).wait_recv()
        sum1[q] = w_ref[:, lanes(2 * place.chip(q) + core)] + cbuf1[q]
        for k in range(3):
            if sent_stage(q, k) == 0:
                red.copy(q, k).start()
    for s in (1, 2, 3):
        red.stage(s)
    for k in range(3):
        ag.start(k)
    ag.run()
    ag.finish()
    for q in range(8):
        to_partner(q).wait_send()
    red.drain()


def wsum(w, token, cid):
    vm = pl.BlockSpec(memory_space=pltpu.VMEM)
    dma = pltpu.SemaphoreType.DMA
    f32 = jnp.float32
    return pl.pallas_call(
        wsum_kernel, out_shape=jax.ShapeDtypeStruct((384, DIM), f32), in_specs=[vm, vm], out_specs=vm,
        scratch_shapes=[pltpu.VMEM((8, 384, 128), f32), pltpu.VMEM((8, 384, 128), f32), pltpu.VMEM((3, 7, 128, 128), f32),
                        dma((2, 8)), dma((3, 8)), dma((3, 24)), dma((3, 24)), dma((3, 8)), dma((3, 8)), dma((3, 8)),
                        dma((3,))],
        compiler_params=pltpu.CompilerParams(collective_id=cid, has_side_effects=True),
        cost_estimate=pl.CostEstimate(flops=20_000_000_000, bytes_accessed=6_000_000, transcendentals=0),
        name='wsum')(w, token)


COLS = ((0, 640), (640, 640), (1280, 768))
TILE = 256


def tile_at(n):
    return pl.ds(pl.multiple_of(n * TILE, TILE), TILE)


def layer_kernel(x_hbm, d_hbm, w_hbm, pre_hbm, vec_ref, init_ref, shard_ref, tot_ref, act_hbm,
                 x_ref, d_ref, w_ref, tile, st, xt, part, cbuf, rbuf, xsem, dwsem, tsem, slots, sems, csem, rs_s, rs_r):
    place = Place()
    me, core = place.me, place.core
    load_d = pltpu.make_async_copy(d_hbm, d_ref, dwsem.at[0])
    load_w = pltpu.make_async_copy(w_hbm, w_ref, dwsem.at[1])

    def load_x(q):
        at = tile_at(place.chip(q))
        return pltpu.make_async_copy(x_hbm.at[:, at], x_ref.at[:, at], xsem.at[q])

    def load_tile(m):
        return pltpu.make_async_copy(pre_hbm.at[pl.ds(m * TILE, TILE)], tile.at[m % 2], tsem.at[0, m % 2])

    def save_tile(m):
        return pltpu.make_async_copy(tile.at[m % 2], act_hbm.at[pl.ds(m * TILE, TILE)], tsem.at[1, m % 2])

    load_x(Q_ORDER[0]).start()
    load_d.start()
    for q in Q_ORDER[1:]:
        load_x(q).start()
    load_w.start()
    load_tile(0).start()
    st[...] = init_ref[...]
    entry_barrier(me)
    small = SmallSum(me, st, tot_ref, slots, sems)

    def to_partner(q):
        return rcopy(part.at[1, q], cbuf.at[q], csem.at[0, q], csem.at[1, q], place.partner)

    def cols(k):
        return pl.ds(*COLS[k])

    red = Reduce(place, lambda q, k: part.at[0, q, :, cols(k)],
                 lambda s, q, k: rbuf.at[k, land_slot(s, q, k), :, pl.ds(0, COLS[k][1])], rs_s, rs_r)

    def core_sum(q):
        to_partner(q).wait_recv()

        @pl.loop(0, 8)
        def _(n):
            at = tile_at(n)
            part[0, q, :, at] = part[0, q, :, at] + cbuf[q, :, at]

        for k in range(3):
            if sent_stage(q, k) == 0:
                red.copy(q, k).start()

    def chunk(m):
        v, s = m // 4, m % 2
        if m > 0:
            save_tile(m - 1).wait()
        if m < 7:
            load_tile(m + 1).start()
        load_tile(m).wait()
        rows = pl.ds(m * TILE, TILE)

        @pl.loop(0, 8)
        def _(n):
            at = tile_at(n)
            grad = lax.dot_general(d_ref[rows, :], w_ref[at, :], (((1,), (1,)), ((), ())),
                                   preferred_element_type=jnp.float32)
            normed = (tile[s, :, at] - vec_ref[pl.ds(v, 1), at]) * vec_ref[pl.ds(2 + v, 1), at]
            act = vec_ref[pl.ds(4, 1), at] * normed + vec_ref[pl.ds(5, 1), at]
            grad = jnp.where(act > 0.0, grad, 0.0)
            tile[s, :, at] = grad
            st[pl.ds(v, 1), at] = st[pl.ds(v, 1), at] + jnp.sum(grad, axis=0, keepdims=True)
            st[pl.ds(2 + v, 1), at] = st[pl.ds(2 + v, 1), at] + jnp.sum(grad * normed, axis=0, keepdims=True)

        save_tile(m).start()

    for i, q in enumerate(Q_ORDER):
        p = place.chip(q)
        load_x(q).wait()

        @pl.loop(0, 8)
        def _(n):
            at = tile_at(n)
            xt[:, at] = jnp.transpose(x_ref[at, tile_at(p)])

        if i == 0:
            load_d.wait()

        @pl.loop(0, 8)
        def _(n):
            at = tile_at(n)
            out = jnp.dot(xt[...], d_ref[:, at], preferred_element_type=jnp.float32)
            part[core, q, :, at] = out[:128]
            part[1 - core, q, :, at] = out[128:]

        to_partner(q).start()
        if i > 0:
            core_sum(Q_ORDER[i - 1])
    load_w.wait()
    chunk(0)
    core_sum(0)
    for m in range(1, 5):
        chunk(m)
    red.stage(1)
    for m in range(5, 8):
        chunk(m)
    small.start()
    red.stage(2)
    small.middle()
    red.stage(3)
    shard_ref[...] = part[0, 0]
    small.finish()
    save_tile(7).wait()
    for q in range(8):
        to_partner(q).wait_send()
    red.drain()


def layer_call(x, d, w, pre, vecs, init, cid):
    vm = pl.BlockSpec(memory_space=pltpu.VMEM)
    hbm = pl.BlockSpec(memory_space=pl.ANY)
    dma = pltpu.SemaphoreType.DMA
    f32, bf16 = jnp.float32, jnp.bfloat16
    rows = 2 * ROWS
    return pl.pallas_call(
        layer_kernel,
        out_shape=(jax.ShapeDtypeStruct((128, DIM), f32), jax.ShapeDtypeStruct((8, DIM), f32),
                   jax.ShapeDtypeStruct((rows, DIM), f32)),
        in_specs=[hbm, hbm, hbm, hbm, vm, vm], out_specs=(vm, vm, hbm),
        scratch_shapes=[pltpu.VMEM((rows, DIM), bf16), pltpu.VMEM((rows, DIM), bf16), pltpu.VMEM((DIM, DIM), bf16),
                        pltpu.VMEM((2, TILE, DIM), f32), pltpu.VMEM((8, DIM), f32), pltpu.VMEM((TILE, rows), bf16),
                        pltpu.VMEM((2, 8, 128, DIM), f32), pltpu.VMEM((8, 128, DIM), f32),
                        pltpu.VMEM((3, 7, 128, 768), f32), dma((8,)), dma((2,)), dma((2, 2))] + SMALL_SCRATCH
                       + [dma((2, 8)), dma((3, 8)), dma((3, 24))],
        compiler_params=pltpu.CompilerParams(collective_id=cid, has_side_effects=True, vmem_limit_bytes=VMEM_LIMIT),
        cost_estimate=pl.CostEstimate(flops=50_000_000_000, bytes_accessed=60_000_000, transcendentals=0),
        name='layer_back')(x, d, w, pre, vecs, init)


def pad_rows(*rows):
    x = jnp.concatenate(rows, axis=0)
    return jnp.pad(x, ((0, 8 - x.shape[0]), (0, 0)))


def layer_forward(x_in, weight, gain_vec, bias_vec, cid):
    pre_act = jnp.einsum('vnk,kd->vnd', x_in, weight, preferred_element_type=jnp.float32)
    moments = small_sum(pad_rows(jnp.sum(pre_act, axis=1), jnp.sum(pre_act * pre_act, axis=1)), cid)
    col_mean = moments[0:2] / ALL_ROWS
    col_var = moments[2:4] / ALL_ROWS - col_mean * col_mean
    inv_std = lax.rsqrt(col_var + BN_EPS)
    normed = (pre_act - col_mean[:, None, :]) * inv_std[:, None, :]
    act_val = gain_vec * normed + bias_vec
    vecs = pad_rows(col_mean, inv_std, gain_vec[None], bias_vec[None])
    return jnp.maximum(act_val, 0.0).astype(jnp.bfloat16), pre_act, normed, inv_std, vecs


def layer_backward(x, d, w, saved, gain_vec, init, cid):
    pre_act, normed, inv_std, vecs = saved
    flat = (2 * ROWS, DIM)
    shard, sums, d_act = layer_call(x.reshape(flat), d.reshape(flat), w, pre_act.reshape(flat), vecs, init, cid)
    mean_d = (sums[0:2] / ALL_ROWS)[:, None, :]
    mean_dn = (sums[2:4] / ALL_ROWS)[:, None, :]
    d_pre = inv_std[:, None, :] * gain_vec * (d_act.reshape(2, ROWS, DIM) - mean_d - normed * mean_dn)
    grad_w = lax.all_gather(shard, 'data', axis=0, tiled=True)
    return d_pre.astype(jnp.bfloat16), grad_w, sums[2] + sums[3], sums[0] + sums[1], sums


def solution(mesh):
    def local_step(h_a, h_b, w_one, w_two, w_three, gain_one, bias_one, gain_two, bias_two):
        view_feats = jnp.stack([h_a, h_b])
        hidden_one, *saved_one = layer_forward(view_feats, w_one, gain_one, bias_one, 0)
        hidden_two, *saved_two = layer_forward(hidden_one, w_two, gain_two, bias_two, 1)
        z_views = jnp.einsum('vnk,kd->vnd', hidden_two, w_three, preferred_element_type=jnp.float32).astype(jnp.bfloat16)
        z_diff = z_views[0].astype(jnp.float32) - z_views[1].astype(jnp.float32)
        stats = pad_rows(jnp.sum(z_views, axis=1, dtype=jnp.float32), jnp.sum(z_diff * z_diff, axis=0)[None])
        d_z, tot, loss_part = gram_loss(z_views, stats, 2)
        loss_row = jnp.pad(jnp.sum(loss_part, axis=0)[None], ((4, 3), (0, DIM - 128)))
        d_pre_two, grad_three, gain_grad_two, bias_grad_two, sums = layer_backward(
            hidden_two, d_z, w_three, saved_two, gain_two, loss_row, 3)
        loss_val = INV_WEIGHT * jnp.sum(tot[2]) / ALL_ROWS + jnp.sum(sums[4])
        d_pre_one, grad_two, gain_grad_one, bias_grad_one, _ = layer_backward(
            hidden_one, d_pre_two, w_two, saved_one, gain_one, jnp.zeros((8, DIM), jnp.float32), 4)
        grad_three, token = place_result(grad_three)
        grad_one = jnp.einsum('vnf,vnd->fd', view_feats, d_pre_one, preferred_element_type=jnp.float32)
        grad_one = wsum(grad_one, token, 5)
        return loss_val, grad_one, grad_two, grad_three, gain_grad_one, bias_grad_one, gain_grad_two, bias_grad_two

    row_spec = P('data', None)
    return jax.shard_map(local_step, mesh=mesh,
                         in_specs=(row_spec, row_spec, P(), P(), P(), P(), P(), P(), P()),
                         out_specs=(P(), P(), P(), P(), P(), P(), P(), P()),
                         check_vma=False)
```
